32 devices in a mesh: seq: 8 (over z, y), rep: 4 (over x, core).
Axes of the slice: x: 2, y: 2, z: 4, core: 2. Of those that a mesh axis runs over, the one named last changes fastest.
Arguments:
- query_rows: bfloat16 [12288, 1024], P(('seq', 'rep')), may hold values from -6 to 6
- key_rows: bfloat16 [12288, 128], P(('seq', 'rep')), may hold values from -6 to 6
- value_rows: bfloat16 [12288, 128], P(('seq', 'rep')), may hold values from -6 to 6
- out_grad: bfloat16 [12288, 1024], P(('seq', 'rep')), may hold values from -1.5 to 1.5
- logsumexp: float32 [8, 12288], P(None, ('seq', 'rep')), may hold values from 1 to 3
- row_delta: float32 [8, 12288], P(None, ('seq', 'rep')), may hold values from -8 to 8
- doc_lengths: int32 [31], replicated, may hold values from 1 to 1537, as said below
Outputs:
- query_grad: bfloat16 [12288, 1024], P(('seq', 'rep'))
- key_grad: bfloat16 [12288, 128], P(('seq', 'rep'))
- value_grad: bfloat16 [12288, 128], P(('seq', 'rep'))
The draws below stay inside these ranges and needn't reach their ends.
Inputs may be any that keep to these rules, and one draw needn't show every extreme that they name: `doc_lengths`: 31 document lengths in pack order, summing to 12288; so every document lies within 5 consecutive aligned blocks of 384 positions.
All inputs are finite; a program needn't handle non-finite values.
Results may differ from the reference program's by a relative error of at most 0.019.
Values may be sent and summed in bfloat16 or wider, within the bound.
A program may use at most 64 MiB of HBM per device.

```python
import jax
import jax.numpy as jnp
from jax import lax

HEADS = 8
HD = 128
TOK_DEV = 384
REACH = 4
TOKENS = 12288
N_SEQ = 8
N_REP = 4


def draw_doc_lengths(key, part):
    blocks = N_SEQ * N_REP
    frames = 2 * blocks // REACH
    span = REACH * TOK_DEV // 2
    short_most = TOK_DEV // 4
    base_key = jax.random.fold_in(key, 11)
    key_start, key_short, key_pick = jax.random.split(base_key, 3)
    starts = jax.random.randint(key_start, (frames + 1,), short_most, span).astype(jnp.int32)
    shorts = jax.random.randint(key_short, (frames + 1,), 1, short_most + 1).astype(jnp.int32)
    chosen = jax.random.randint(key_pick, (), 1, frames - 1).astype(jnp.int32)
    index = jnp.arange(frames + 1, dtype=jnp.int32)
    starts = jnp.where(index == chosen + 1, span - 1, starts)
    starts = jnp.where(index == chosen - 1, jnp.minimum(starts, span - 4 - short_most), starts)
    starts = jnp.where(index == chosen, -3, starts)
    shorts = jnp.where(index == chosen + 1, 1, shorts)
    starts = jnp.where((index == 0) | (index == frames), 0, starts)
    long_start = index * span + starts
    short_start = long_start - shorts
    inner = jnp.stack([short_start[1:frames], long_start[1:frames]], 1).reshape(-1)
    bounds = jnp.concatenate([jnp.zeros((1,), jnp.int32), inner.astype(jnp.int32), jnp.full((1,), TOKENS, jnp.int32)])
    return (bounds[1:] - bounds[:-1]).astype(jnp.int32)


def block_levels(rng, shape, cuts, low, largest):
    def one(position, blocks):
        steps = jax.random.uniform(jax.random.fold_in(jax.random.fold_in(rng, 6), position), (blocks,), jnp.float32, low / len(cuts), largest / len(cuts))
        return jnp.repeat(jnp.exp(steps), shape[position] // blocks).reshape((-1,) + (1,) * (len(shape) - position - 1))

    gain = one(*cuts[0])
    for cut in cuts[1:]:
        gain = gain * one(*cut)
    return gain


def centred(key, dims, width, most, cuts=(), kind=jnp.bfloat16):
    values = width * jax.random.normal(key, dims, jnp.float32)
    if cuts:
        values = values * block_levels(key, dims, cuts, -0.22, 0.18)
    return jnp.clip(values, -most, most).astype(kind)


def setup_inputs(seed: int = 0) -> dict:
    seeds = jax.random.split(jax.random.key(seed), 8)
    query_rows = centred(seeds[0], (TOKENS, HEADS * HD), 1.0, 6.0, ((0, 32),))
    key_rows = centred(seeds[1], (TOKENS, HD), 1.0, 6.0, ((0, 32),))
    value_rows = centred(seeds[2], (TOKENS, HD), 1.0, 6.0, ((0, 32),))
    out_grad = centred(seeds[3], (TOKENS, HEADS * HD), 0.25, 1.5, ((0, 32),))
    logsumexp = jnp.clip(1.0 + 2.0 * jax.random.uniform(seeds[4], (HEADS, TOKENS), jnp.float32) ** block_levels(seeds[4], (HEADS, TOKENS), ((1, 32),), -0.2, 0.2), 1.0, 3.0)
    row_delta = centred(seeds[5], (HEADS, TOKENS), 2.0, 8.0, ((1, 32),), jnp.float32)
    doc_lengths = draw_doc_lengths(jax.random.fold_in(seeds[7], 71), 0)
    return {"query_rows": query_rows, "key_rows": key_rows, "value_rows": value_rows, "out_grad": out_grad, "logsumexp": logsumexp, "row_delta": row_delta, "doc_lengths": doc_lengths}


def block_grads(query_block, grad_block, stat_block, delta_block, key_block, value_block, query_docs, key_docs, query_pos, key_pos):
    row_count = query_block.shape[0]
    query_heads = query_block.astype(jnp.float32).reshape(row_count, HEADS, HD)
    grad_heads = grad_block.astype(jnp.float32).reshape(row_count, HEADS, HD)
    key_float = key_block.astype(jnp.float32)
    value_float = value_block.astype(jnp.float32)
    score_scale = HD ** -0.5
    scores = jnp.einsum("qhd,kd->hqk", query_heads, key_float) * score_scale
    allowed = (query_docs[:, None] == key_docs[None, :]) & (key_pos[None, :] <= query_pos[:, None])
    probs = jnp.where(allowed[None], jnp.exp(scores - stat_block[:, :, None]), 0.0)
    dprobs = jnp.einsum("qhd,kd->hqk", grad_heads, value_float)
    dscores = probs * (dprobs - delta_block[:, :, None])
    probs_half = probs.astype(jnp.bfloat16).astype(jnp.float32)
    dscores_half = dscores.astype(jnp.bfloat16).astype(jnp.float32)
    query_part = (jnp.einsum("hqk,kd->qhd", dscores_half, key_float) * score_scale).reshape(row_count, HEADS * HD)
    key_part = jnp.einsum("hqk,qhd->kd", dscores_half, query_heads) * score_scale
    value_part = jnp.einsum("hqk,qhd->kd", probs_half, grad_heads)
    return query_part, key_part, value_part


def shifted_blocks(array, distance, filler):
    return jnp.concatenate([filler, array[:-distance]], 0)


def reference(query_rows, key_rows, value_rows, out_grad, logsumexp, row_delta, doc_lengths):
    blocks = N_SEQ * N_REP
    total = blocks * TOK_DEV
    doc_ends = jnp.cumsum(doc_lengths).astype(jnp.int32)
    marks = jnp.zeros((total,), jnp.int32).at[doc_ends[:-1]].add(1)
    docs = jnp.cumsum(marks).astype(jnp.int32).reshape(blocks, TOK_DEV)
    positions = jnp.arange(total, dtype=jnp.int32).reshape(blocks, TOK_DEV)
    queries = query_rows.reshape(blocks, TOK_DEV, HEADS * HD)
    grads = out_grad.reshape(blocks, TOK_DEV, HEADS * HD)
    keys_all = key_rows.reshape(blocks, TOK_DEV, HD)
    values_all = value_rows.reshape(blocks, TOK_DEV, HD)
    stats = logsumexp.reshape(HEADS, blocks, TOK_DEV).transpose(1, 0, 2)
    deltas = row_delta.reshape(HEADS, blocks, TOK_DEV).transpose(1, 0, 2)
    prev_keys = jnp.stack([shifted_blocks(keys_all, step, jnp.zeros_like(keys_all[:step])) for step in range(1, REACH + 1)], 1)
    prev_values = jnp.stack([shifted_blocks(values_all, step, jnp.zeros_like(values_all[:step])) for step in range(1, REACH + 1)], 1)
    prev_docs = jnp.stack([shifted_blocks(docs, step, jnp.full((step, TOK_DEV), -1, jnp.int32)) for step in range(1, REACH + 1)], 1)
    prev_pos = jnp.stack([positions - step * TOK_DEV for step in range(1, REACH + 1)], 1)

    def one_block(block_items):
        query_block, grad_block, stat_block, delta_block, key_block, value_block, doc_block, pos_block, pkey, pvalue, pdoc, ppos = block_items
        query_sum, local_k, local_v = block_grads(query_block, grad_block, stat_block, delta_block, key_block, value_block, doc_block, doc_block, pos_block, pos_block)
        cross_keys = []
        cross_values = []
        for step in range(REACH):
            cross_q, cross_k, cross_v = block_grads(query_block, grad_block, stat_block, delta_block, pkey[step], pvalue[step], doc_block, pdoc[step], pos_block, ppos[step])
            query_sum = query_sum + cross_q
            cross_keys.append(cross_k)
            cross_values.append(cross_v)
        return query_sum, local_k, local_v, jnp.stack(cross_keys, 0), jnp.stack(cross_values, 0)

    query_sum, local_k, local_v, cross_k, cross_v = lax.map(one_block, (queries, grads, stats, deltas, keys_all, values_all, docs, positions, prev_keys, prev_values, prev_docs, prev_pos))
    key_sum = local_k
    value_sum = local_v
    for step in range(1, REACH + 1):
        key_sum = key_sum + jnp.concatenate([cross_k[step:, step - 1], jnp.zeros_like(cross_k[:step, step - 1])], 0)
        value_sum = value_sum + jnp.concatenate([cross_v[step:, step - 1], jnp.zeros_like(cross_v[:step, step - 1])], 0)
    return (query_sum.reshape(total, HEADS * HD).astype(jnp.bfloat16), key_sum.reshape(total, HD).astype(jnp.bfloat16), value_sum.reshape(total, HD).astype(jnp.bfloat16))
```

```python
import functools
import math

import jax
import jax.numpy as jnp
from jax import lax
from jax.experimental import pallas as pl
from jax.experimental.pallas import tpu as pltpu
from jax.sharding import PartitionSpec as P

REACH = 4
LANES = 128
LOG2E = math.log2(math.e)
MESH = pl.DeviceIdType.MESH
MIB = 1024 * 1024


def dot(a, b):
    return jnp.dot(a, b, preferred_element_type=jnp.float32)


def dot_nt(a, b):
    return lax.dot_general(a, b, (((1,), (1,)), ((), ())), preferred_element_type=jnp.float32)


def turned(a):
    return a.astype(jnp.float32).T.astype(jnp.bfloat16)


def kernel(
    count,
    per_seq,
    lens_hbm,
    q_hbm,
    g_hbm,
    k_hbm,
    v_hbm,
    lse_hbm,
    delta_hbm,
    dq_ref,
    dk_ref,
    dv_ref,
    lens,
    q,
    g,
    qt,
    gt,
    own,
    kv,
    k_t,
    bias,
    lse,
    delta,
    lse_row,
    delta_row,
    dq_t,
    own_acc,
    acc,
    out,
    part,
    ret,
    load_sem,
    small_sem,
    kv_send,
    kv_recv,
    part_send,
    part_recv,
    ret_send,
    ret_recv,
):
    rows, head = k_hbm.shape
    heads = q_hbm.shape[1] // head
    pack = 2 if heads % 2 == 0 else 1
    tile = LANES if rows % LANES == 0 else rows
    wide = rows // (2 * tile) * (2 * tile)
    scale = head**-0.5
    me = lax.axis_index("seq") * per_seq + lax.axis_index("rep")
    core = lax.rem(me, 2)
    partner = me + 1 - 2 * core

    def device(index):
        return (lax.div(index, per_seq), lax.rem(index, per_seq))

    def when(*conditions):
        return pl.when(functools.reduce(jnp.logical_and, conditions))

    barrier = pltpu.get_barrier_semaphore()

    def greet(target):
        pl.semaphore_signal(barrier, inc=1, device_id=device(target), device_id_type=MESH)

    greet(partner)
    for d in (2, 4):
        pl.when(me + d < count)(functools.partial(greet, me + d))
        pl.when(me >= d)(functools.partial(greet, me - d))

    small = [
        pltpu.make_async_copy(src, dst, small_sem.at[n])
        for n, (src, dst) in enumerate(
            (
                (lens_hbm, lens),
                (k_hbm, own.at[0]),
                (v_hbm, own.at[1]),
                (lse_hbm, lse),
                (delta_hbm, delta),
            )
        )
    ]
    loads = [
        [
            pltpu.make_async_copy(
                src.at[:, h * head : (h + 1) * head],
                dst.at[h * rows : (h + 1) * rows, :],
                load_sem.at[n, h],
            )
            for n, (src, dst) in enumerate(((q_hbm, q), (g_hbm, g)))
        ]
        for h in range(heads)
    ]
    for copy in small:
        copy.start()
    for pair in loads:
        for copy in pair:
            copy.start()

    def remote(src, dst, send_sem, recv_sem, target):
        return pltpu.make_async_remote_copy(
            src_ref=src,
            dst_ref=dst,
            send_sem=send_sem,
            recv_sem=recv_sem,
            device_id=device(target),
            device_id_type=MESH,
        )

    def kv_copy(src, slot, order, target):
        return remote(src, kv.at[slot], kv_send.at[order], kv_recv.at[slot], target)

    def part_copy(step, slot):
        return remote(out.at[step], part.at[slot], part_send.at[slot], part_recv.at[slot], partner)

    def ret_copy(step, d):
        n = d // 2 - 1
        return remote(out.at[step], ret.at[n], ret_send.at[n], ret_recv.at[n], me - d)

    send_partner = kv_copy(own, 0, 2, partner)
    send_near = kv_copy(own, 3 * core, 0, me + 2)
    send_far = kv_copy(own, 3 - core, 1, me + 4)

    for copy in small[1:3]:
        copy.wait()
    pl.semaphore_wait(
        barrier,
        1 + jnp.minimum(me, REACH) // 2 + jnp.minimum(count - 1 - me, REACH) // 2,
    )

    @when(core == 0)
    def _():
        send_partner.start()

    @when(core == 1, me + 4 < count)
    def _():
        send_far.start()

    @when(me + 2 < count)
    def _():
        send_near.start()

    @when(core == 0, me + 4 < count)
    def _():
        send_far.start()

    small[0].wait()
    t_pos = me * rows + lax.broadcasted_iota(jnp.int32, (1, rows), 1)
    docs = lens.shape[1]
    upto = lax.broadcasted_iota(jnp.int32, (docs, docs), 1) <= lax.broadcasted_iota(
        jnp.int32, (docs, docs), 0
    )
    ends = jnp.sum(jnp.where(upto, lens[...].astype(jnp.float32), 0.0), axis=1, keepdims=True)
    begun = jnp.where(ends <= t_pos.astype(jnp.float32), ends, 0.0)
    start = jnp.max(begun, axis=0, keepdims=True).astype(jnp.int32)
    for copy in small[3:]:
        copy.wait()
    for h in range(heads):
        c = slice(h * rows, (h + 1) * rows)
        lse_row[:, c] = lse[h : h + 1, :] * LOG2E
        delta_row[:, c] = delta[h : h + 1, :]

    def set_bias(d):
        u_pos = (me - d) * rows + lax.broadcasted_iota(jnp.int32, (rows, rows), 0)
        bias[...] = jnp.where((u_pos >= start) & (u_pos <= t_pos), 0.0, -1e30)

    def stack(ref, pieces):
        return jnp.concatenate([ref[h * rows + t : h * rows + t + n, :] for h, t, n in pieces], axis=0)

    def line(ref, pieces):
        return jnp.concatenate([ref[:, h * rows + t : h * rows + t + n] for h, t, n in pieces], axis=1)

    def put(ref, index, value, fresh):
        ref[index] = value if fresh else ref[index] + value

    def scores(k_ref, v_ref, item):
        pieces, low, high = item
        u = slice(low, high)
        return dot_nt(k_ref[u, :], stack(q, pieces)), dot_nt(v_ref[u, :], stack(g, pieces))

    def finish(item, s, dp, acc_ref, seen, first_dq):
        pieces, low, high = item
        u = slice(low, high)
        mask = jnp.concatenate([bias[u, t : t + n] for _, t, n in pieces], axis=1)
        p = jnp.exp2(s * (scale * LOG2E) + (mask - line(lse_row, pieces)))
        ds = (p * (dp - line(delta_row, pieces))).astype(jnp.bfloat16)
        p = p.astype(jnp.bfloat16)
        for n, (weight, turned_rows, plain_rows) in enumerate(((ds, qt, q), (p, gt, g))):
            if low < wide:
                top = min(high, wide)
                part_t = dot_nt(line(turned_rows, pieces), weight[: top - low, :])
                for i in range(low // tile, top // tile):
                    at = i * tile - low
                    put(acc_ref, (n, i), part_t[:, at : at + tile], (n, i) not in seen)
                    seen.add((n, i))
            if high > wide:
                base = max(low, wide)
                part_n = dot(weight[base - low :, :], stack(plain_rows, pieces))
                for i in range(base // tile, high // tile):
                    at = i * tile - base
                    put(acc_ref, (n, i), part_n[at : at + tile, :], (n, i) not in seen)
                    seen.add((n, i))
        dq = dot(k_t[:, u], ds)
        at = 0
        for h, t, n in pieces:
            put(dq_t, (slice(None), slice(h * rows + t, h * rows + t + n)), dq[:, at : at + n], first_dq)
            at += n

    def sweep(k_ref, v_ref, items, acc_ref, first_dq, before=None):
        seen = set()
        held = None
        for n, item in enumerate(items):
            if before is not None:
                before(n)
            ahead = scores(k_ref, v_ref, item)
            if held is not None:
                finish(*held, acc_ref, seen, first_dq)
            held = (item, *ahead)
        finish(*held, acc_ref, seen, first_dq)

    def runs(begin, width):
        pieces = []
        while width:
            t = begin % rows
            n = min(width, rows - t)
            pieces.append((begin // rows, t, n))
            begin, width = begin + n, width - n
        return pieces

    span = 2 * tile
    full_items = [(runs(b, span), 0, rows) for b in range(0, heads * rows, span)]
    pairs = [[h + m for m in range(pack)] for h in range(0, heads, pack)]
    own_items = [
        ([(h, t, tile) for h in pair], 0, t + tile) for pair in pairs for t in reversed(range(0, rows, tile))
    ]
    far_items = [([(h, t, tile) for h in pair], t, rows) for pair in pairs for t in range(0, rows, tile)]

    set_bias(0)
    k_t[...] = turned(own[0])

    def bring(n):
        if n % (rows // tile) == 0:
            for h in pairs[n // (rows // tile)]:
                for copy in loads[h]:
                    copy.wait()
                c = slice(h * rows, (h + 1) * rows)
                qt[:, c] = turned(q[c, :])
                gt[:, c] = turned(g[c, :])

    sweep(own.at[0], own.at[1], own_items, own_acc, True, bring)

    def round_out(step):
        out[step] = acc[step].astype(jnp.bfloat16)

    def merge_out(step, slot, d):
        part_copy(step, slot).wait_recv()
        out[step] = (acc[step] + part[slot].astype(jnp.float32)).astype(jnp.bfloat16)
        ret_copy(step, d).start()

    def arrive(slot):
        kv_copy(own, slot, 0, partner).wait_recv()

    def step_body(step, carry):
        even = step + 2 - lax.div(step, 2) * (7 - 2 * step)
        odd = 2 * step + 1 - lax.div(step, 2) * (4 * step - 7)
        d = even + core * (odd - even)

        @when(core == 0, me >= d)
        def _():
            arrive(step)

        @when(core == 0, step == 0, me >= 2)
        def _():
            kv_copy(kv.at[0], 1, 3, partner).start()

        @when(core == 1, step == 0)
        def _():
            arrive(0)

        @when(core == 1, step == 1, me >= 4)
        def _():
            arrive(2)
            kv_copy(kv.at[2], 1, 4, partner).start()

        @when(core == 1, step == 1, me >= 3)
        def _():
            arrive(1)

        @when(core == 1, step == 2, me >= 2)
        def _():
            arrive(3)
            kv_copy(kv.at[3], 2, 3, partner).start()

        @when(me >= d)
        def _():
            set_bias(d)
            k_t[...] = turned(kv[step, 0])

            @when(d == REACH)
            def _():
                sweep(kv.at[step, 0], kv.at[step, 1], far_items, acc.at[step], False)

            @when(d != REACH)
            def _():
                sweep(kv.at[step, 0], kv.at[step, 1], full_items, acc.at[step], False)

        @when(core == 0, step == 1, me >= 3)
        def _():
            round_out(1)
            part_copy(1, 1).start()

        @when(core == 0, step == 1, me >= 2)
        def _():
            merge_out(0, 0, 2)

        @when(core == 0, step == 2, me >= 1)
        def _():
            round_out(2)
            part_copy(2, 0).start()

        @when(core == 0, step == 3, me >= 4)
        def _():
            round_out(3)
            ret_copy(3, 4).start()

        @when(core == 1, step == 0)
        def _():
            round_out(0)
            part_copy(0, 1).start()

        @when(core == 1, step == 1, me >= 3)
        def _():
            round_out(1)
            part_copy(1, 0).start()

        @when(core == 1, step == 3, me >= 4)
        def _():
            merge_out(2, 1, 4)

        @when(core == 1, step == 3, me >= 2)
        def _():
            merge_out(3, 0, 2)

        return carry

    lax.fori_loop(0, REACH, step_body, 0)

    for h in range(heads):
        c = slice(h * head, (h + 1) * head)
        dq_ref[:, c] = (dq_t[:, h * rows : (h + 1) * rows] * scale).T.astype(jnp.bfloat16)

    @when(core == 0)
    def _():
        part_copy(1, 1).wait_recv()
        own_acc[...] = own_acc[...] + part[1].astype(jnp.float32)

    for d in (2, 4):

        @when(me + d < count)
        def _():
            ret_copy(0, d).wait_recv()
            own_acc[...] = own_acc[...] + ret[d // 2 - 1].astype(jnp.float32)

    for i in range(rows // tile):
        r = slice(i * tile, (i + 1) * tile)
        dk = own_acc[0, i] * scale
        dv = own_acc[1, i]
        dk_ref[r, :] = (dk.T if i * tile < wide else dk).astype(jnp.bfloat16)
        dv_ref[r, :] = (dv.T if i * tile < wide else dv).astype(jnp.bfloat16)

    @when(me + 2 < count)
    def _():
        send_near.wait_send()

    @when(me + 4 < count)
    def _():
        send_far.wait_send()

    @when(core == 0)
    def _():
        send_partner.wait_send()

    @when(me >= 2)
    def _():
        kv_copy(kv.at[0], 1, 3, partner).wait_send()
        part_copy(0, 0).wait_send()
        ret_copy(0, 2).wait_send()

    @when(me >= 4)
    def _():
        ret_copy(0, 4).wait_send()

    @when(core == 1, me >= 4)
    def _():
        kv_copy(kv.at[2], 1, 4, partner).wait_send()

    @when((core == 1) | (me >= 4))
    def _():
        part_copy(0, 1).wait_send()


def pass_on(dq_ref, dk_ref, dv_ref, dq_out, dk_out, dv_out, sem):
    copies = [
        pltpu.make_async_copy(src, dst, sem.at[n])
        for n, (src, dst) in enumerate(((dq_ref, dq_out), (dk_ref, dk_out), (dv_ref, dv_out)))
    ]
    for copy in copies:
        copy.start()
    for copy in copies:
        copy.wait()


def shards(count, per_seq, query_rows, key_rows, value_rows, out_grad, logsumexp, row_delta, doc_lengths):
    rows, head = key_rows.shape
    wide = query_rows.shape
    heads = wide[1] // head
    sums = (2, rows // LANES, LANES, head)
    half, full = jnp.bfloat16, jnp.float32
    vmem = pl.BlockSpec(memory_space=pltpu.VMEM)
    hbm = pl.BlockSpec(memory_space=pl.ANY)
    operands = [
        pltpu.with_memory_space_constraint(x, pltpu.HBM)
        for x in (doc_lengths.reshape(1, -1), query_rows, out_grad, key_rows, value_rows, logsumexp, row_delta)
    ]
    grads = pl.pallas_call(
        functools.partial(kernel, count, per_seq),
        out_shape=(
            jax.ShapeDtypeStruct(wide, half),
            jax.ShapeDtypeStruct((rows, head), half),
            jax.ShapeDtypeStruct((rows, head), half),
        ),
        in_specs=[hbm] * 7,
        out_specs=(vmem, vmem, vmem),
        scratch_shapes=[
            pltpu.VMEM((1, doc_lengths.shape[0]), jnp.int32),
            pltpu.VMEM((heads * rows, head), half),
            pltpu.VMEM((heads * rows, head), half),
            pltpu.VMEM((head, heads * rows), half),
            pltpu.VMEM((head, heads * rows), half),
            pltpu.VMEM((2, rows, head), half),
            pltpu.VMEM((REACH, 2, rows, head), half),
            pltpu.VMEM((head, rows), half),
            pltpu.VMEM((rows, rows), full),
            pltpu.VMEM(logsumexp.shape, full),
            pltpu.VMEM(row_delta.shape, full),
            pltpu.VMEM((1, heads * rows), full),
            pltpu.VMEM((1, heads * rows), full),
            pltpu.VMEM((head, heads * rows), full),
            pltpu.VMEM(sums, full),
            pltpu.VMEM((REACH, *sums), full),
            pltpu.VMEM((REACH, *sums), half),
            pltpu.VMEM((2, *sums), half),
            pltpu.VMEM((2, *sums), half),
            pltpu.SemaphoreType.DMA((2, heads)),
            pltpu.SemaphoreType.DMA((5,)),
            pltpu.SemaphoreType.DMA((5,)),
            pltpu.SemaphoreType.DMA((REACH,)),
            pltpu.SemaphoreType.DMA((2,)),
            pltpu.SemaphoreType.DMA((2,)),
            pltpu.SemaphoreType.DMA((2,)),
            pltpu.SemaphoreType.DMA((2,)),
        ],
        compiler_params=pltpu.CompilerParams(
            collective_id=0, has_side_effects=True, vmem_limit_bytes=40 * MIB
        ),
    )(*operands)
    return pl.pallas_call(
        pass_on,
        out_shape=tuple(jax.ShapeDtypeStruct(x.shape, x.dtype) for x in grads),
        in_specs=[vmem] * 3,
        out_specs=(hbm,) * 3,
        scratch_shapes=[pltpu.SemaphoreType.DMA((3,))],
        compiler_params=pltpu.CompilerParams(vmem_limit_bytes=8 * MIB),
    )(*grads)


def solution(mesh):
    both = ("seq", "rep")
    count = mesh.shape["seq"] * mesh.shape["rep"]
    return jax.shard_map(
        functools.partial(shards, count, mesh.shape["rep"]),
        mesh=mesh,
        in_specs=(
            P(both, None),
            P(both, None),
            P(both, None),
            P(both, None),
            P(None, both),
            P(None, both),
            P(),
        ),
        out_specs=(P(both, None), P(both, None), P(both, None)),
        check_vma=False,
    )
```

```python
import functools
import math

import jax
import jax.numpy as jnp
from jax import lax
from jax.experimental import pallas as pl
from jax.experimental.pallas import tpu as pltpu
from jax.sharding import PartitionSpec as P

REACH = 4
LANES = 128
LOG2E = math.log2(math.e)
MESH = pl.DeviceIdType.MESH
MIB = 1024 * 1024


def dot(a, b):
    return jnp.dot(a, b, preferred_element_type=jnp.float32)


def dot_nt(a, b):
    return lax.dot_general(a, b, (((1,), (1,)), ((), ())), preferred_element_type=jnp.float32)


def turned(a):
    return a.astype(jnp.float32).T.astype(jnp.bfloat16)


def kernel(
    count,
    per_seq,
    lens_hbm,
    q_hbm,
    g_hbm,
    k_hbm,
    v_hbm,
    lse_hbm,
    delta_hbm,
    dq_ref,
    dk_ref,
    dv_ref,
    lens,
    q,
    g,
    qt,
    gt,
    own,
    kv,
    k_t,
    bias,
    lse,
    delta,
    lse_row,
    delta_row,
    dq_t,
    own_acc,
    acc,
    out,
    part,
    ret,
    load_sem,
    small_sem,
    kv_send,
    kv_recv,
    part_send,
    part_recv,
    ret_send,
    ret_recv,
):
    rows, head = k_hbm.shape
    heads = q_hbm.shape[1] // head
    pack = 2 if heads % 2 == 0 else 1
    tile = LANES if rows % LANES == 0 else rows
    wide = rows // (2 * tile) * (2 * tile)
    scale = head**-0.5
    me = lax.axis_index("seq") * per_seq + lax.axis_index("rep")
    core = lax.rem(me, 2)
    partner = me + 1 - 2 * core

    def device(index):
        return (lax.div(index, per_seq), lax.rem(index, per_seq))

    def when(*conditions):
        return pl.when(functools.reduce(jnp.logical_and, conditions))

    small = [
        pltpu.make_async_copy(src, dst, small_sem.at[n])
        for n, (src, dst) in enumerate(
            (
                (k_hbm, own.at[0]),
                (v_hbm, own.at[1]),
                (lens_hbm, lens),
                (lse_hbm, lse),
                (delta_hbm, delta),
            )
        )
    ]
    loads = [
        [
            pltpu.make_async_copy(
                src.at[:, h * head : (h + 1) * head],
                dst.at[h * rows : (h + 1) * rows, :],
                load_sem.at[n, h],
            )
            for n, (src, dst) in enumerate(((q_hbm, q), (g_hbm, g)))
        ]
        for h in range(heads)
    ]
    for copy in small:
        copy.start()

    barrier = pltpu.get_barrier_semaphore()

    def greet(target):
        pl.semaphore_signal(barrier, inc=1, device_id=device(target), device_id_type=MESH)

    greet(partner)
    for d in (2, 4):
        pl.when(me + d < count)(functools.partial(greet, me + d))
        pl.when(me >= d)(functools.partial(greet, me - d))

    def remote(src, dst, send_sem, recv_sem, target):
        return pltpu.make_async_remote_copy(
            src_ref=src,
            dst_ref=dst,
            send_sem=send_sem,
            recv_sem=recv_sem,
            device_id=device(target),
            device_id_type=MESH,
        )

    def kv_copy(src, slot, order, target):
        return remote(src, kv.at[slot], kv_send.at[order], kv_recv.at[slot], target)

    def part_copy(step, slot):
        return remote(out.at[step], part.at[slot], part_send.at[slot], part_recv.at[slot], partner)

    def ret_copy(step, d):
        n = d // 2 - 1
        return remote(out.at[step], ret.at[n], ret_send.at[n], ret_recv.at[n], me - d)

    send_partner = kv_copy(own, 0, 2, partner)
    send_near = kv_copy(own, 3 * core, 0, me + 2)
    send_far = kv_copy(own, 3 - core, 1, me + 4)

    for copy in small[:2]:
        copy.wait()
    for pair in loads:
        for copy in pair:
            copy.start()
    pl.semaphore_wait(
        barrier,
        1 + jnp.minimum(me, REACH) // 2 + jnp.minimum(count - 1 - me, REACH) // 2,
    )

    @when(core == 0)
    def _():
        send_partner.start()

    @when(core == 0, me + 2 < count)
    def _():
        send_near.start()

    small[2].wait()
    t_pos = me * rows + lax.broadcasted_iota(jnp.int32, (1, rows), 1)
    docs = lens.shape[1]
    upto = lax.broadcasted_iota(jnp.int32, (docs, docs), 1) <= lax.broadcasted_iota(
        jnp.int32, (docs, docs), 0
    )
    ends = jnp.sum(jnp.where(upto, lens[...].astype(jnp.float32), 0.0), axis=1, keepdims=True)
    begun = jnp.where(ends <= t_pos.astype(jnp.float32), ends, 0.0)
    start = jnp.max(begun, axis=0, keepdims=True).astype(jnp.int32)
    for copy in small[3:]:
        copy.wait()
    for h in range(heads):
        c = slice(h * rows, (h + 1) * rows)
        lse_row[:, c] = lse[h : h + 1, :] * LOG2E
        delta_row[:, c] = delta[h : h + 1, :]

    def set_bias(d):
        u_pos = (me - d) * rows + lax.broadcasted_iota(jnp.int32, (rows, rows), 0)
        bias[...] = jnp.where((u_pos >= start) & (u_pos <= t_pos), 0.0, -1e30)

    def stack(ref, pieces):
        return jnp.concatenate([ref[h * rows + t : h * rows + t + n, :] for h, t, n in pieces], axis=0)

    def line(ref, pieces):
        return jnp.concatenate([ref[:, h * rows + t : h * rows + t + n] for h, t, n in pieces], axis=1)

    def put(ref, index, value, fresh):
        ref[index] = value if fresh else ref[index] + value

    def scores(k_ref, v_ref, item):
        pieces, low, high = item
        u = slice(low, high)
        return dot_nt(k_ref[u, :], stack(q, pieces)), dot_nt(v_ref[u, :], stack(g, pieces))

    def finish(item, s, dp, acc_ref, seen, first_dq):
        pieces, low, high = item
        u = slice(low, high)
        mask = jnp.concatenate([bias[u, t : t + n] for _, t, n in pieces], axis=1)
        p = jnp.exp2(s * (scale * LOG2E) + (mask - line(lse_row, pieces)))
        ds = (p * (dp - line(delta_row, pieces))).astype(jnp.bfloat16)
        p = p.astype(jnp.bfloat16)
        for n, (weight, turned_rows, plain_rows) in enumerate(((ds, qt, q), (p, gt, g))):
            if low < wide:
                top = min(high, wide)
                part_t = dot_nt(line(turned_rows, pieces), weight[: top - low, :])
                for i in range(low // tile, top // tile):
                    at = i * tile - low
                    put(acc_ref, (n, i), part_t[:, at : at + tile], (n, i) not in seen)
                    seen.add((n, i))
            if high > wide:
                base = max(low, wide)
                part_n = dot(weight[base - low :, :], stack(plain_rows, pieces))
                for i in range(base // tile, high // tile):
                    at = i * tile - base
                    put(acc_ref, (n, i), part_n[at : at + tile, :], (n, i) not in seen)
                    seen.add((n, i))
        dq = dot(k_t[:, u], ds)
        at = 0
        for h, t, n in pieces:
            put(dq_t, (slice(None), slice(h * rows + t, h * rows + t + n)), dq[:, at : at + n], first_dq)
            at += n

    def sweep(k_ref, v_ref, items, acc_ref, first_dq, before=None):
        seen = set()
        held = None
        for n, item in enumerate(items):
            if before is not None:
                before(n)
            ahead = scores(k_ref, v_ref, item)
            if held is not None:
                finish(*held, acc_ref, seen, first_dq)
            held = (item, *ahead)
        finish(*held, acc_ref, seen, first_dq)

    def runs(begin, width):
        pieces = []
        while width:
            t = begin % rows
            n = min(width, rows - t)
            pieces.append((begin // rows, t, n))
            begin, width = begin + n, width - n
        return pieces

    span = 2 * tile
    full_items = [(runs(b, span), 0, rows) for b in range(0, heads * rows, span)]
    pairs = [[h + m for m in range(pack)] for h in range(0, heads, pack)]
    own_items = [
        ([(h, t, tile) for h in pair], 0, t + tile) for pair in pairs for t in reversed(range(0, rows, tile))
    ]
    far_items = [([(h, t, tile) for h in pair], t, rows) for pair in pairs for t in range(0, rows, tile)]

    set_bias(0)
    k_t[...] = turned(own[0])

    def bring(n):
        if n % (rows // tile) == 0:
            for h in pairs[n // (rows // tile)]:
                for copy in loads[h]:
                    copy.wait()
                c = slice(h * rows, (h + 1) * rows)
                qt[:, c] = turned(q[c, :])
                gt[:, c] = turned(g[c, :])

    sweep(own.at[0], own.at[1], own_items, own_acc, True, bring)

    @when(core == 1, me + 4 < count)
    def _():
        send_far.start()

    def round_out(step):
        out[step] = acc[step].astype(jnp.bfloat16)

    def merge_out(step, slot, d):
        part_copy(step, slot).wait_recv()
        out[step] = (acc[step] + part[slot].astype(jnp.float32)).astype(jnp.bfloat16)
        ret_copy(step, d).start()

    def arrive(slot):
        kv_copy(own, slot, 0, partner).wait_recv()

    def step_body(step, carry):
        even = step + 2 - lax.div(step, 2) * (7 - 2 * step)
        odd = 2 * step + 1 - lax.div(step, 2) * (4 * step - 7)
        d = even + core * (odd - even)

        @when(core == 0, me >= d)
        def _():
            arrive(step)

        @when(core == 0, step == 0, me >= 2)
        def _():
            kv_copy(kv.at[0], 1, 3, partner).start()

        @when(core == 1, step == 0)
        def _():
            arrive(0)

        @when(core == 1, step == 1, me >= 4)
        def _():
            arrive(2)
            kv_copy(kv.at[2], 1, 4, partner).start()

        @when(core == 1, step == 1, me >= 3)
        def _():
            arrive(1)

        @when(core == 1, step == 2, me >= 2)
        def _():
            arrive(3)
            kv_copy(kv.at[3], 2, 3, partner).start()

        @when(me >= d)
        def _():
            set_bias(d)
            k_t[...] = turned(kv[step, 0])

            @when(d == REACH)
            def _():
                sweep(kv.at[step, 0], kv.at[step, 1], far_items, acc.at[step], False)

            @when(d != REACH)
            def _():
                sweep(kv.at[step, 0], kv.at[step, 1], full_items, acc.at[step], False)

        @when(core == 1, step == 0, me + 2 < count)
        def _():
            send_near.start()

        @when(core == 0, step == 0, me + 4 < count)
        def _():
            send_far.start()

        @when(core == 0, step == 1, me >= 4)
        def _():
            round_out(1)
            part_copy(1, 1).start()

        @when(core == 0, step == 1, me >= 2)
        def _():
            merge_out(0, 0, 2)

        @when(core == 0, step == 2, me >= 2)
        def _():
            round_out(2)
            part_copy(2, 0).start()

        @when(core == 0, step == 3, me >= 4)
        def _():
            round_out(3)
            ret_copy(3, 4).start()

        @when(core == 1, step == 0)
        def _():
            round_out(0)
            part_copy(0, 1).start()

        @when(core == 1, step == 1, me >= 3)
        def _():
            round_out(1)
            part_copy(1, 0).start()

        @when(core == 1, step == 2, me >= 4)
        def _():
            merge_out(2, 1, 4)

        @when(core == 1, step == 3, me >= 2)
        def _():
            merge_out(3, 0, 2)

        return carry

    lax.fori_loop(0, REACH, step_body, 0)

    for h in range(heads):
        c = slice(h * head, (h + 1) * head)
        dq_ref[:, c] = (dq_t[:, h * rows : (h + 1) * rows] * scale).T.astype(jnp.bfloat16)

    @when(core == 0)
    def _():
        part_copy(1, 1).wait_recv()
        own_acc[...] = own_acc[...] + part[1].astype(jnp.float32)

    for d in (2, 4):

        @when(me + d < count)
        def _():
            ret_copy(0, d).wait_recv()
            own_acc[...] = own_acc[...] + ret[d // 2 - 1].astype(jnp.float32)

    for i in range(rows // tile):
        r = slice(i * tile, (i + 1) * tile)
        dk = own_acc[0, i] * scale
        dv = own_acc[1, i]
        dk_ref[r, :] = (dk.T if i * tile < wide else dk).astype(jnp.bfloat16)
        dv_ref[r, :] = (dv.T if i * tile < wide else dv).astype(jnp.bfloat16)

    @when(me + 2 < count)
    def _():
        send_near.wait_send()

    @when(me + 4 < count)
    def _():
        send_far.wait_send()

    @when(core == 0)
    def _():
        send_partner.wait_send()

    @when(me >= 2)
    def _():
        kv_copy(kv.at[0], 1, 3, partner).wait_send()
        part_copy(0, 0).wait_send()
        ret_copy(0, 2).wait_send()

    @when(me >= 4)
    def _():
        ret_copy(0, 4).wait_send()

    @when(core == 1, me >= 4)
    def _():
        kv_copy(kv.at[2], 1, 4, partner).wait_send()

    @when((core == 1) | (me >= 4))
    def _():
        part_copy(0, 1).wait_send()


def pass_on(dq_ref, dk_ref, dv_ref, dq_out, dk_out, dv_out, sem):
    copies = [
        pltpu.make_async_copy(src, dst, sem.at[n])
        for n, (src, dst) in enumerate(((dq_ref, dq_out), (dk_ref, dk_out), (dv_ref, dv_out)))
    ]
    for copy in copies:
        copy.start()
    for copy in copies:
        copy.wait()


def shards(count, per_seq, query_rows, key_rows, value_rows, out_grad, logsumexp, row_delta, doc_lengths):
    rows, head = key_rows.shape
    wide = query_rows.shape
    heads = wide[1] // head
    sums = (2, rows // LANES, LANES, head)
    half, full = jnp.bfloat16, jnp.float32
    vmem = pl.BlockSpec(memory_space=pltpu.VMEM)
    hbm = pl.BlockSpec(memory_space=pl.ANY)
    operands = [
        pltpu.with_memory_space_constraint(x, pltpu.HBM)
        for x in (doc_lengths.reshape(1, -1), query_rows, out_grad, key_rows, value_rows, logsumexp, row_delta)
    ]
    grads = pl.pallas_call(
        functools.partial(kernel, count, per_seq),
        out_shape=(
            jax.ShapeDtypeStruct(wide, half),
            jax.ShapeDtypeStruct((rows, head), half),
            jax.ShapeDtypeStruct((rows, head), half),
        ),
        in_specs=[hbm] * 7,
        out_specs=(vmem, vmem, vmem),
        scratch_shapes=[
            pltpu.VMEM((1, doc_lengths.shape[0]), jnp.int32),
            pltpu.VMEM((heads * rows, head), half),
            pltpu.VMEM((heads * rows, head), half),
            pltpu.VMEM((head, heads * rows), half),
            pltpu.VMEM((head, heads * rows), half),
            pltpu.VMEM((2, rows, head), half),
            pltpu.VMEM((REACH, 2, rows, head), half),
            pltpu.VMEM((head, rows), half),
            pltpu.VMEM((rows, rows), full),
            pltpu.VMEM(logsumexp.shape, full),
            pltpu.VMEM(row_delta.shape, full),
            pltpu.VMEM((1, heads * rows), full),
            pltpu.VMEM((1, heads * rows), full),
            pltpu.VMEM((head, heads * rows), full),
            pltpu.VMEM(sums, full),
            pltpu.VMEM((REACH, *sums), full),
            pltpu.VMEM((REACH, *sums), half),
            pltpu.VMEM((2, *sums), half),
            pltpu.VMEM((2, *sums), half),
            pltpu.SemaphoreType.DMA((2, heads)),
            pltpu.SemaphoreType.DMA((5,)),
            pltpu.SemaphoreType.DMA((5,)),
            pltpu.SemaphoreType.DMA((REACH,)),
            pltpu.SemaphoreType.DMA((2,)),
            pltpu.SemaphoreType.DMA((2,)),
            pltpu.SemaphoreType.DMA((2,)),
            pltpu.SemaphoreType.DMA((2,)),
        ],
        compiler_params=pltpu.CompilerParams(
            collective_id=0, has_side_effects=True, vmem_limit_bytes=40 * MIB
        ),
    )(*operands)
    return pl.pallas_call(
        pass_on,
        out_shape=tuple(jax.ShapeDtypeStruct(x.shape, x.dtype) for x in grads),
        in_specs=[vmem] * 3,
        out_specs=(hbm,) * 3,
        scratch_shapes=[pltpu.SemaphoreType.DMA((3,))],
        compiler_params=pltpu.CompilerParams(vmem_limit_bytes=8 * MIB),
    )(*grads)


def solution(mesh):
    both = ("seq", "rep")
    count = mesh.shape["seq"] * mesh.shape["rep"]
    return jax.shard_map(
        functools.partial(shards, count, mesh.shape["rep"]),
        mesh=mesh,
        in_specs=(
            P(both, None),
            P(both, None),
            P(both, None),
            P(both, None),
            P(None, both),
            P(None, both),
            P(),
        ),
        out_specs=(P(both, None), P(both, None), P(both, None)),
        check_vma=False,
    )
```

```python
import functools
import math

import jax
import jax.numpy as jnp
from jax import lax
from jax.experimental import pallas as pl
from jax.experimental.pallas import tpu as pltpu
from jax.sharding import PartitionSpec as P

REACH = 4
LANES = 128
LOG2E = math.log2(math.e)
MESH = pl.DeviceIdType.MESH
MIB = 1024 * 1024


def dot(a, b):
    return jnp.dot(a, b, preferred_element_type=jnp.float32)


def dot_nt(a, b):
    return lax.dot_general(a, b, (((1,), (1,)), ((), ())), preferred_element_type=jnp.float32)


def turned(a):
    return a.astype(jnp.float32).T.astype(jnp.bfloat16)


def kernel(
    count,
    per_seq,
    lens_hbm,
    q_hbm,
    g_hbm,
    k_hbm,
    v_hbm,
    lse_hbm,
    delta_hbm,
    dq_ref,
    dk_ref,
    dv_ref,
    lens,
    q,
    g,
    qt,
    gt,
    own,
    kv,
    k_t,
    bias,
    lse,
    delta,
    lse_row,
    delta_row,
    dq_t,
    own_acc,
    acc,
    out,
    part,
    ret,
    load_sem,
    small_sem,
    kv_send,
    kv_recv,
    part_send,
    part_recv,
    ret_send,
    ret_recv,
):
    rows, head = k_hbm.shape
    heads = q_hbm.shape[1] // head
    pack = 2 if heads % 2 == 0 else 1
    tile = LANES if rows % LANES == 0 else rows
    wide = rows // (2 * tile) * (2 * tile)
    scale = head**-0.5
    me = lax.axis_index("seq") * per_seq + lax.axis_index("rep")
    core = lax.rem(me, 2)
    partner = me + 1 - 2 * core
    crossing = lax.rem(me, 8)

    def device(index):
        return (lax.div(index, per_seq), lax.rem(index, per_seq))

    def when(*conditions):
        return pl.when(functools.reduce(jnp.logical_and, conditions))

    small = [
        pltpu.make_async_copy(src, dst, small_sem.at[n])
        for n, (src, dst) in enumerate(
            (
                (k_hbm, own.at[0]),
                (v_hbm, own.at[1]),
                (lens_hbm, lens),
                (lse_hbm, lse),
                (delta_hbm, delta),
            )
        )
    ]
    loads = [
        [
            pltpu.make_async_copy(
                src.at[:, h * head : (h + 1) * head],
                dst.at[h * rows : (h + 1) * rows, :],
                load_sem.at[n, h],
            )
            for n, (src, dst) in enumerate(((q_hbm, q), (g_hbm, g)))
        ]
        for h in range(heads)
    ]
    for copy in small:
        copy.start()

    barrier = pltpu.get_barrier_semaphore()

    def greet(target):
        pl.semaphore_signal(barrier, inc=1, device_id=device(target), device_id_type=MESH)

    greet(partner)
    for d in (2, 4):
        pl.when(me + d < count)(functools.partial(greet, me + d))
        pl.when(me >= d)(functools.partial(greet, me - d))

    def remote(src, dst, send_sem, recv_sem, target):
        return pltpu.make_async_remote_copy(
            src_ref=src,
            dst_ref=dst,
            send_sem=send_sem,
            recv_sem=recv_sem,
            device_id=device(target),
            device_id_type=MESH,
        )

    def kv_copy(src, slot, order, target):
        return remote(src, kv.at[slot], kv_send.at[order], kv_recv.at[slot], target)

    def part_copy(step, slot):
        return remote(out.at[step], part.at[slot], part_send.at[slot], part_recv.at[slot], partner)

    def ret_copy(step, d):
        n = d // 2 - 1
        return remote(out.at[step], ret.at[n], ret_send.at[n], ret_recv.at[n], me - d)

    send_partner = kv_copy(own, 0, 2, partner)
    send_near = kv_copy(own, 3 * core, 0, me + 2)
    send_far = kv_copy(own, 3 - core, 1, me + 4)

    for copy in small[:2]:
        copy.wait()
    for pair in loads:
        for copy in pair:
            copy.start()
    pl.semaphore_wait(
        barrier,
        1 + jnp.minimum(me, REACH) // 2 + jnp.minimum(count - 1 - me, REACH) // 2,
    )

    @when(core == 0)
    def _():
        send_partner.start()

    @when(core == 0, me + 2 < count)
    def _():
        send_near.start()

    small[2].wait()
    t_pos = me * rows + lax.broadcasted_iota(jnp.int32, (1, rows), 1)
    docs = lens.shape[1]
    upto = lax.broadcasted_iota(jnp.int32, (docs, docs), 1) <= lax.broadcasted_iota(
        jnp.int32, (docs, docs), 0
    )
    ends = jnp.sum(jnp.where(upto, lens[...].astype(jnp.float32), 0.0), axis=1, keepdims=True)
    begun = jnp.where(ends <= t_pos.astype(jnp.float32), ends, 0.0)
    start = jnp.max(begun, axis=0, keepdims=True).astype(jnp.int32)
    for copy in small[3:]:
        copy.wait()
    for h in range(heads):
        c = slice(h * rows, (h + 1) * rows)
        lse_row[:, c] = lse[h : h + 1, :] * LOG2E
        delta_row[:, c] = delta[h : h + 1, :]

    def set_bias(d):
        u_pos = (me - d) * rows + lax.broadcasted_iota(jnp.int32, (rows, rows), 0)
        bias[...] = jnp.where((u_pos >= start) & (u_pos <= t_pos), 0.0, -1e30)

    def stack(ref, pieces):
        return jnp.concatenate([ref[h * rows + t : h * rows + t + n, :] for h, t, n in pieces], axis=0)

    def line(ref, pieces):
        return jnp.concatenate([ref[:, h * rows + t : h * rows + t + n] for h, t, n in pieces], axis=1)

    def put(ref, index, value, fresh):
        ref[index] = value if fresh else ref[index] + value

    def scores(k_ref, v_ref, item):
        pieces, low, high = item
        u = slice(low, high)
        return dot_nt(k_ref[u, :], stack(q, pieces)), dot_nt(v_ref[u, :], stack(g, pieces))

    def finish(item, s, dp, acc_ref, seen, first_dq):
        pieces, low, high = item
        u = slice(low, high)
        mask = jnp.concatenate([bias[u, t : t + n] for _, t, n in pieces], axis=1)
        p = jnp.exp2(s * (scale * LOG2E) + (mask - line(lse_row, pieces)))
        ds = (p * (dp - line(delta_row, pieces))).astype(jnp.bfloat16)
        p = p.astype(jnp.bfloat16)
        for n, (weight, turned_rows, plain_rows) in enumerate(((ds, qt, q), (p, gt, g))):
            if low < wide:
                top = min(high, wide)
                part_t = dot_nt(line(turned_rows, pieces), weight[: top - low, :])
                for i in range(low // tile, top // tile):
                    at = i * tile - low
                    put(acc_ref, (n, i), part_t[:, at : at + tile], (n, i) not in seen)
                    seen.add((n, i))
            if high > wide:
                base = max(low, wide)
                part_n = dot(weight[base - low :, :], stack(plain_rows, pieces))
                for i in range(base // tile, high // tile):
                    at = i * tile - base
                    put(acc_ref, (n, i), part_n[at : at + tile, :], (n, i) not in seen)
                    seen.add((n, i))
        dq = dot(k_t[:, u], ds)
        at = 0
        for h, t, n in pieces:
            put(dq_t, (slice(None), slice(h * rows + t, h * rows + t + n)), dq[:, at : at + n], first_dq)
            at += n

    def sweep(k_ref, v_ref, items, acc_ref, first_dq, before=None):
        seen = set()
        held = None
        for n, item in enumerate(items):
            if before is not None:
                before(n)
            ahead = scores(k_ref, v_ref, item)
            if held is not None:
                finish(*held, acc_ref, seen, first_dq)
            held = (item, *ahead)
        finish(*held, acc_ref, seen, first_dq)

    def runs(begin, width):
        pieces = []
        while width:
            t = begin % rows
            n = min(width, rows - t)
            pieces.append((begin // rows, t, n))
            begin, width = begin + n, width - n
        return pieces

    span = 2 * tile
    full_items = [(runs(b, span), 0, rows) for b in range(0, heads * rows, span)]
    pairs = [[h + m for m in range(pack)] for h in range(0, heads, pack)]
    own_items = [
        ([(h, t, tile) for h in pair], 0, t + tile) for pair in pairs for t in reversed(range(0, rows, tile))
    ]
    far_items = [([(h, t, tile) for h in pair], t, rows) for pair in pairs for t in range(0, rows, tile)]

    set_bias(0)
    k_t[...] = turned(own[0])

    def bring(n):
        if n % (rows // tile) == 0:
            for h in pairs[n // (rows // tile)]:
                for copy in loads[h]:
                    copy.wait()
                c = slice(h * rows, (h + 1) * rows)
                qt[:, c] = turned(q[c, :])
                gt[:, c] = turned(g[c, :])

    sweep(own.at[0], own.at[1], own_items, own_acc, True, bring)

    @when(core == 1, me + 4 < count)
    def _():
        send_far.start()

    @when(core == 1, crossing != 3, me + 2 < count)
    def _():
        send_near.start()

    def round_out(step):
        out[step] = acc[step].astype(jnp.bfloat16)

    def merge_out(step, slot, d):
        part_copy(step, slot).wait_recv()
        out[step] = (acc[step] + part[slot].astype(jnp.float32)).astype(jnp.bfloat16)
        ret_copy(step, d).start()

    def arrive(slot):
        kv_copy(own, slot, 0, partner).wait_recv()

    def step_body(step, carry):
        even = step + 2 - lax.div(step, 2) * (7 - 2 * step)
        odd = 2 * step + 1 - lax.div(step, 2) * (4 * step - 7)
        d = even + core * (odd - even)

        @when(core == 0, me >= d)
        def _():
            arrive(step)

        @when(core == 0, step == 0, me >= 2)
        def _():
            kv_copy(kv.at[0], 1, 3, partner).start()

        @when(core == 1, step == 0)
        def _():
            arrive(0)

        @when(core == 1, step == 1, me >= 4)
        def _():
            arrive(2)
            kv_copy(kv.at[2], 1, 4, partner).start()

        @when(core == 1, step == 1, me >= 3)
        def _():
            arrive(1)

        @when(core == 1, step == 2, me >= 2)
        def _():
            arrive(3)
            kv_copy(kv.at[3], 2, 3, partner).start()

        @when(me >= d)
        def _():
            set_bias(d)
            k_t[...] = turned(kv[step, 0])

            @when(d == REACH)
            def _():
                sweep(kv.at[step, 0], kv.at[step, 1], far_items, acc.at[step], False)

            @when(d != REACH)
            def _():
                sweep(kv.at[step, 0], kv.at[step, 1], full_items, acc.at[step], False)

        @when(core == 1, step == 0, crossing == 3, me + 2 < count)
        def _():
            send_near.start()

        @when(core == 0, step == 0, me >= 2, me + 4 < count)
        def _():
            send_far.start()

        @when(core == 0, step == 1, me >= 4)
        def _():
            round_out(1)
            part_copy(1, 1).start()

        @when(core == 0, step == 1, me >= 2)
        def _():
            merge_out(0, 0, 2)

        @when(core == 0, step == 2, me >= 2)
        def _():
            round_out(2)
            part_copy(2, 0).start()

        @when(core == 0, step == 3, me >= 4)
        def _():
            round_out(3)
            ret_copy(3, 4).start()

        @when(core == 1, step == 0)
        def _():
            round_out(0)
            part_copy(0, 1).start()

        @when(core == 1, step == 1, me >= 3)
        def _():
            round_out(1)
            part_copy(1, 0).start()

        @when(core == 1, step == 2, me >= 4)
        def _():
            merge_out(2, 1, 4)

        @when(core == 1, step == 3, me >= 2)
        def _():
            merge_out(3, 0, 2)

        return carry

    lax.fori_loop(0, REACH, step_body, 0)

    for h in range(heads):
        c = slice(h * head, (h + 1) * head)
        dq_ref[:, c] = (dq_t[:, h * rows : (h + 1) * rows] * scale).T.astype(jnp.bfloat16)

    @when(core == 0)
    def _():
        part_copy(1, 1).wait_recv()

        @when(me < 2, me + 4 < count)
        def _():
            send_far.start()

        own_acc[...] = own_acc[...] + part[1].astype(jnp.float32)

    for d in (2, 4):

        @when(me + d < count)
        def _():
            ret_copy(0, d).wait_recv()
            own_acc[...] = own_acc[...] + ret[d // 2 - 1].astype(jnp.float32)

    for i in range(rows // tile):
        r = slice(i * tile, (i + 1) * tile)
        dk = own_acc[0, i] * scale
        dv = own_acc[1, i]
        dk_ref[r, :] = (dk.T if i * tile < wide else dk).astype(jnp.bfloat16)
        dv_ref[r, :] = (dv.T if i * tile < wide else dv).astype(jnp.bfloat16)

    @when(me + 2 < count)
    def _():
        send_near.wait_send()

    @when(me + 4 < count)
    def _():
        send_far.wait_send()

    @when(core == 0)
    def _():
        send_partner.wait_send()

    @when(me >= 2)
    def _():
        kv_copy(kv.at[0], 1, 3, partner).wait_send()
        part_copy(0, 0).wait_send()
        ret_copy(0, 2).wait_send()

    @when(me >= 4)
    def _():
        ret_copy(0, 4).wait_send()

    @when(core == 1, me >= 4)
    def _():
        kv_copy(kv.at[2], 1, 4, partner).wait_send()

    @when((core == 1) | (me >= 4))
    def _():
        part_copy(0, 1).wait_send()


def pass_on(dq_ref, dk_ref, dv_ref, dq_out, dk_out, dv_out, sem):
    copies = [
        pltpu.make_async_copy(src, dst, sem.at[n])
        for n, (src, dst) in enumerate(((dq_ref, dq_out), (dk_ref, dk_out), (dv_ref, dv_out)))
    ]
    for copy in copies:
        copy.start()
    for copy in copies:
        copy.wait()


def shards(count, per_seq, query_rows, key_rows, value_rows, out_grad, logsumexp, row_delta, doc_lengths):
    rows, head = key_rows.shape
    wide = query_rows.shape
    heads = wide[1] // head
    sums = (2, rows // LANES, LANES, head)
    half, full = jnp.bfloat16, jnp.float32
    vmem = pl.BlockSpec(memory_space=pltpu.VMEM)
    hbm = pl.BlockSpec(memory_space=pl.ANY)
    operands = [
        pltpu.with_memory_space_constraint(x, pltpu.HBM)
        for x in (doc_lengths.reshape(1, -1), query_rows, out_grad, key_rows, value_rows, logsumexp, row_delta)
    ]
    grads = pl.pallas_call(
        functools.partial(kernel, count, per_seq),
        out_shape=(
            jax.ShapeDtypeStruct(wide, half),
            jax.ShapeDtypeStruct((rows, head), half),
            jax.ShapeDtypeStruct((rows, head), half),
        ),
        in_specs=[hbm] * 7,
        out_specs=(vmem, vmem, vmem),
        scratch_shapes=[
            pltpu.VMEM((1, doc_lengths.shape[0]), jnp.int32),
            pltpu.VMEM((heads * rows, head), half),
            pltpu.VMEM((heads * rows, head), half),
            pltpu.VMEM((head, heads * rows), half),
            pltpu.VMEM((head, heads * rows), half),
            pltpu.VMEM((2, rows, head), half),
            pltpu.VMEM((REACH, 2, rows, head), half),
            pltpu.VMEM((head, rows), half),
            pltpu.VMEM((rows, rows), full),
            pltpu.VMEM(logsumexp.shape, full),
            pltpu.VMEM(row_delta.shape, full),
            pltpu.VMEM((1, heads * rows), full),
            pltpu.VMEM((1, heads * rows), full),
            pltpu.VMEM((head, heads * rows), full),
            pltpu.VMEM(sums, full),
            pltpu.VMEM((REACH, *sums), full),
            pltpu.VMEM((REACH, *sums), half),
            pltpu.VMEM((2, *sums), half),
            pltpu.VMEM((2, *sums), half),
            pltpu.SemaphoreType.DMA((2, heads)),
            pltpu.SemaphoreType.DMA((5,)),
            pltpu.SemaphoreType.DMA((5,)),
            pltpu.SemaphoreType.DMA((REACH,)),
            pltpu.SemaphoreType.DMA((2,)),
            pltpu.SemaphoreType.DMA((2,)),
            pltpu.SemaphoreType.DMA((2,)),
            pltpu.SemaphoreType.DMA((2,)),
        ],
        compiler_params=pltpu.CompilerParams(
            collective_id=0, has_side_effects=True, vmem_limit_bytes=40 * MIB
        ),
    )(*operands)
    return pl.pallas_call(
        pass_on,
        out_shape=tuple(jax.ShapeDtypeStruct(x.shape, x.dtype) for x in grads),
        in_specs=[vmem] * 3,
        out_specs=(hbm,) * 3,
        scratch_shapes=[pltpu.SemaphoreType.DMA((3,))],
        compiler_params=pltpu.CompilerParams(vmem_limit_bytes=8 * MIB),
    )(*grads)


def solution(mesh):
    both = ("seq", "rep")
    count = mesh.shape["seq"] * mesh.shape["rep"]
    return jax.shard_map(
        functools.partial(shards, count, mesh.shape["rep"]),
        mesh=mesh,
        in_specs=(
            P(both, None),
            P(both, None),
            P(both, None),
            P(both, None),
            P(None, both),
            P(None, both),
            P(),
        ),
        out_specs=(P(both, None), P(both, None), P(both, None)),
        check_vma=False,
    )
```

```python
import functools
import math

import jax
import jax.numpy as jnp
from jax import lax
from jax.experimental import pallas as pl
from jax.experimental.pallas import tpu as pltpu
from jax.sharding import PartitionSpec as P

REACH = 4
LANES = 128
LOG2E = math.log2(math.e)
MESH = pl.DeviceIdType.MESH
MIB = 1024 * 1024


def dot(a, b):
    return jnp.dot(a, b, preferred_element_type=jnp.float32)


def dot_nt(a, b):
    return lax.dot_general(a, b, (((1,), (1,)), ((), ())), preferred_element_type=jnp.float32)


def turned(a):
    return a.astype(jnp.float32).T.astype(jnp.bfloat16)


def kernel(
    count,
    per_seq,
    lens_hbm,
    q_hbm,
    g_hbm,
    k_hbm,
    v_hbm,
    lse_hbm,
    delta_hbm,
    dq_ref,
    dk_ref,
    dv_ref,
    lens,
    q,
    g,
    qt,
    gt,
    own,
    kv,
    k_t,
    bias,
    lse,
    delta,
    lse_row,
    delta_row,
    dq_t,
    own_acc,
    acc,
    out,
    part,
    ret,
    load_sem,
    small_sem,
    kv_send,
    kv_recv,
    part_send,
    part_recv,
    ret_send,
    ret_recv,
):
    rows, head = k_hbm.shape
    heads = q_hbm.shape[1] // head
    pack = 2 if heads % 2 == 0 else 1
    tile = LANES if rows % LANES == 0 else rows
    wide = rows // (2 * tile) * (2 * tile)
    scale = head**-0.5
    me = lax.axis_index("seq") * per_seq + lax.axis_index("rep")
    core = lax.rem(me, 2)
    partner = me + 1 - 2 * core
    crossing = lax.rem(me, 8)

    def device(index):
        return (lax.div(index, per_seq), lax.rem(index, per_seq))

    def when(*conditions):
        return pl.when(functools.reduce(jnp.logical_and, conditions))

    small = [
        pltpu.make_async_copy(src, dst, small_sem.at[n])
        for n, (src, dst) in enumerate(
            (
                (k_hbm, own.at[0]),
                (v_hbm, own.at[1]),
                (lens_hbm, lens),
                (lse_hbm, lse),
                (delta_hbm, delta),
            )
        )
    ]
    loads = [
        [
            pltpu.make_async_copy(
                src.at[:, h * head : (h + 1) * head],
                dst.at[h * rows : (h + 1) * rows, :],
                load_sem.at[n, h],
            )
            for n, (src, dst) in enumerate(((q_hbm, q), (g_hbm, g)))
        ]
        for h in range(heads)
    ]
    for copy in small:
        copy.start()

    barrier = pltpu.get_barrier_semaphore()

    def greet(target):
        pl.semaphore_signal(barrier, inc=1, device_id=device(target), device_id_type=MESH)

    greet(partner)
    for d in (2, 4):
        pl.when(me + d < count)(functools.partial(greet, me + d))
        pl.when(me >= d)(functools.partial(greet, me - d))

    def remote(src, dst, send_sem, recv_sem, target):
        return pltpu.make_async_remote_copy(
            src_ref=src,
            dst_ref=dst,
            send_sem=send_sem,
            recv_sem=recv_sem,
            device_id=device(target),
            device_id_type=MESH,
        )

    def kv_copy(src, slot, order, target):
        return remote(src, kv.at[slot], kv_send.at[order], kv_recv.at[slot], target)

    def part_copy(step, slot):
        return remote(out.at[step], part.at[slot], part_send.at[slot], part_recv.at[slot], partner)

    parts = [(wide // tile, rows // tile), (0, wide // tile)]

    def ret_copies(step, d):
        if d == 2:
            return [remote(out.at[step], ret.at[0], ret_send.at[0], ret_recv.at[0], me - d)]
        return [
            remote(
                out.at[step, :, i:j],
                ret.at[1, :, i:j],
                ret_send.at[1 + n],
                ret_recv.at[1 + n],
                me - d,
            )
            for n, (i, j) in enumerate(parts)
        ]

    send_partner = kv_copy(own, 0, 2, partner)
    send_near = kv_copy(own, 3 * core, 0, me + 2)
    send_far = kv_copy(own, 3 - core, 1, me + 4)

    for copy in small[:2]:
        copy.wait()
    for pair in loads:
        for copy in pair:
            copy.start()
    pl.semaphore_wait(
        barrier,
        1 + jnp.minimum(me, REACH) // 2 + jnp.minimum(count - 1 - me, REACH) // 2,
    )

    @when(core == 0)
    def _():
        send_partner.start()

    @when(core == 0, me + 2 < count)
    def _():
        send_near.start()

    small[2].wait()
    t_pos = me * rows + lax.broadcasted_iota(jnp.int32, (1, rows), 1)
    docs = lens.shape[1]
    upto = lax.broadcasted_iota(jnp.int32, (docs, docs), 1) <= lax.broadcasted_iota(
        jnp.int32, (docs, docs), 0
    )
    ends = jnp.sum(jnp.where(upto, lens[...].astype(jnp.float32), 0.0), axis=1, keepdims=True)
    begun = jnp.where(ends <= t_pos.astype(jnp.float32), ends, 0.0)
    start = jnp.max(begun, axis=0, keepdims=True).astype(jnp.int32)
    for copy in small[3:]:
        copy.wait()
    for h in range(heads):
        c = slice(h * rows, (h + 1) * rows)
        lse_row[:, c] = lse[h : h + 1, :] * LOG2E
        delta_row[:, c] = delta[h : h + 1, :]

    def set_bias(d):
        u_pos = (me - d) * rows + lax.broadcasted_iota(jnp.int32, (rows, rows), 0)
        bias[...] = jnp.where((u_pos >= start) & (u_pos <= t_pos), 0.0, -1e30)

    def stack(ref, pieces):
        return jnp.concatenate([ref[h * rows + t : h * rows + t + n, :] for h, t, n in pieces], axis=0)

    def line(ref, pieces):
        return jnp.concatenate([ref[:, h * rows + t : h * rows + t + n] for h, t, n in pieces], axis=1)

    def put(ref, index, value, fresh):
        ref[index] = value if fresh else ref[index] + value

    def scores(k_ref, v_ref, item):
        pieces, low, high = item
        u = slice(low, high)
        return dot_nt(k_ref[u, :], stack(q, pieces)), dot_nt(v_ref[u, :], stack(g, pieces))

    def finish(item, s, dp, acc_ref, seen, first_dq):
        pieces, low, high = item
        u = slice(low, high)
        mask = jnp.concatenate([bias[u, t : t + n] for _, t, n in pieces], axis=1)
        p = jnp.exp2(s * (scale * LOG2E) + (mask - line(lse_row, pieces)))
        ds = (p * (dp - line(delta_row, pieces))).astype(jnp.bfloat16)
        p = p.astype(jnp.bfloat16)
        for n, (weight, turned_rows, plain_rows) in enumerate(((ds, qt, q), (p, gt, g))):
            if low < wide:
                top = min(high, wide)
                part_t = dot_nt(line(turned_rows, pieces), weight[: top - low, :])
                for i in range(low // tile, top // tile):
                    at = i * tile - low
                    put(acc_ref, (n, i), part_t[:, at : at + tile], (n, i) not in seen)
                    seen.add((n, i))
            if high > wide:
                base = max(low, wide)
                part_n = dot(weight[base - low :, :], stack(plain_rows, pieces))
                for i in range(base // tile, high // tile):
                    at = i * tile - base
                    put(acc_ref, (n, i), part_n[at : at + tile, :], (n, i) not in seen)
                    seen.add((n, i))
        dq = dot(k_t[:, u], ds)
        at = 0
        for h, t, n in pieces:
            put(dq_t, (slice(None), slice(h * rows + t, h * rows + t + n)), dq[:, at : at + n], first_dq)
            at += n

    def sweep(k_ref, v_ref, items, acc_ref, first_dq, before=None, depth=1):
        seen = set()
        held = []
        for n, item in enumerate(items):
            if before is not None:
                before(n)
            held.append((item, *scores(k_ref, v_ref, item)))
            if len(held) > depth:
                finish(*held.pop(0), acc_ref, seen, first_dq)
        for rest in held:
            finish(*rest, acc_ref, seen, first_dq)

    def runs(begin, width):
        pieces = []
        while width:
            t = begin % rows
            n = min(width, rows - t)
            pieces.append((begin // rows, t, n))
            begin, width = begin + n, width - n
        return pieces

    span = 2 * tile
    full_items = [(runs(b, span), 0, rows) for b in range(0, heads * rows, span)]
    pairs = [[h + m for m in range(pack)] for h in range(0, heads, pack)]
    own_items = [
        ([(h, t, tile) for h in pair], 0, t + tile) for pair in pairs for t in reversed(range(0, rows, tile))
    ]
    far_items = [([(h, t, tile) for h in pair], t, rows) for pair in pairs for t in range(0, rows, tile)]
    late_items = [(pieces, max(low, wide), rows) for pieces, low, _ in far_items]
    early_items = [(pieces, low, wide) for pieces, low, _ in far_items if low < wide]

    set_bias(0)
    k_t[...] = turned(own[0])

    def bring(n):
        if n % (rows // tile) == 0:
            for h in pairs[n // (rows // tile)]:
                for copy in loads[h]:
                    copy.wait()
                c = slice(h * rows, (h + 1) * rows)
                qt[:, c] = turned(q[c, :])
                gt[:, c] = turned(g[c, :])

    sweep(own.at[0], own.at[1], own_items, own_acc, True, bring)

    @when(core == 1, me + 4 < count)
    def _():
        send_far.start()

    @when(core == 1, crossing != 3, me + 2 < count)
    def _():
        send_near.start()

    def round_out(step):
        out[step] = acc[step].astype(jnp.bfloat16)

    def merge_out(step, slot, d):
        part_copy(step, slot).wait_recv()
        out[step] = (acc[step] + part[slot].astype(jnp.float32)).astype(jnp.bfloat16)
        for copy in ret_copies(step, d):
            copy.start()

    def arrive(slot):
        kv_copy(own, slot, 0, partner).wait_recv()

    def step_body(step, carry):
        even = step + 2 - lax.div(step, 2) * (7 - 2 * step)
        odd = 2 * step + 1 - lax.div(step, 2) * (4 * step - 7)
        d = even + core * (odd - even)

        @when(core == 0, me >= d)
        def _():
            arrive(step)

        @when(core == 0, step == 0, me >= 2)
        def _():
            kv_copy(kv.at[0], 1, 3, partner).start()

        @when(core == 1, step == 0)
        def _():
            arrive(0)

        @when(core == 1, step == 1, me >= 4)
        def _():
            arrive(2)
            kv_copy(kv.at[2], 1, 4, partner).start()

        @when(core == 1, step == 1, me >= 3)
        def _():
            arrive(1)

        @when(core == 1, step == 2, me >= 2)
        def _():
            arrive(3)
            kv_copy(kv.at[3], 2, 3, partner).start()

        @when(me >= d)
        def _():
            set_bias(d)
            k_t[...] = turned(kv[step, 0])

            @when(d == REACH)
            def _():
                @when(core == 1)
                def _():
                    sweep(kv.at[2, 0], kv.at[2, 1], far_items, acc.at[2], False)

                @when(core == 0)
                def _():
                    todo = zip(ret_copies(3, 4), (late_items, early_items), parts, (2, 1))
                    for copy, items, (i, j), depth in todo:
                        sweep(kv.at[3, 0], kv.at[3, 1], items, acc.at[3], False, depth=depth)
                        out[3, :, i:j] = acc[3, :, i:j].astype(jnp.bfloat16)
                        copy.start()

            @when(d != REACH)
            def _():
                sweep(kv.at[step, 0], kv.at[step, 1], full_items, acc.at[step], False)

        @when(core == 1, step == 0, crossing == 3, me + 2 < count)
        def _():
            send_near.start()

        @when(core == 0, step == 0, me >= 2, me + 4 < count)
        def _():
            send_far.start()

        @when(core == 0, step == 1, me >= 4)
        def _():
            round_out(1)
            part_copy(1, 1).start()

        @when(core == 0, step == 1, me >= 2)
        def _():
            merge_out(0, 0, 2)

        @when(core == 0, step == 2, me >= 2)
        def _():
            round_out(2)
            part_copy(2, 0).start()

        @when(core == 1, step == 0)
        def _():
            round_out(0)
            part_copy(0, 1).start()

        @when(core == 1, step == 1, me >= 3)
        def _():
            round_out(1)
            part_copy(1, 0).start()

        @when(core == 1, step == 2, me >= 4)
        def _():
            merge_out(2, 1, 4)

        @when(core == 1, step == 3, me >= 2)
        def _():
            merge_out(3, 0, 2)

        return carry

    lax.fori_loop(0, REACH, step_body, 0)

    for h in range(heads):
        c = slice(h * head, (h + 1) * head)
        dq_ref[:, c] = (dq_t[:, h * rows : (h + 1) * rows] * scale).T.astype(jnp.bfloat16)

    @when(core == 0)
    def _():
        part_copy(1, 1).wait_recv()

        @when(me < 2, me + 4 < count)
        def _():
            send_far.start()

        own_acc[...] = own_acc[...] + part[1].astype(jnp.float32)

    for d in (2, 4):

        @when(me + d < count)
        def _():
            for copy in ret_copies(0, d):
                copy.wait_recv()
            own_acc[...] = own_acc[...] + ret[d // 2 - 1].astype(jnp.float32)

    for i in range(rows // tile):
        r = slice(i * tile, (i + 1) * tile)
        dk = own_acc[0, i] * scale
        dv = own_acc[1, i]
        dk_ref[r, :] = (dk.T if i * tile < wide else dk).astype(jnp.bfloat16)
        dv_ref[r, :] = (dv.T if i * tile < wide else dv).astype(jnp.bfloat16)

    @when(me + 2 < count)
    def _():
        send_near.wait_send()

    @when(me + 4 < count)
    def _():
        send_far.wait_send()

    @when(core == 0)
    def _():
        send_partner.wait_send()

    @when(me >= 2)
    def _():
        kv_copy(kv.at[0], 1, 3, partner).wait_send()
        part_copy(0, 0).wait_send()
        for copy in ret_copies(0, 2):
            copy.wait_send()

    @when(me >= 4)
    def _():
        for copy in ret_copies(0, 4):
            copy.wait_send()

    @when(core == 1, me >= 4)
    def _():
        kv_copy(kv.at[2], 1, 4, partner).wait_send()

    @when((core == 1) | (me >= 4))
    def _():
        part_copy(0, 1).wait_send()


def pass_on(dq_ref, dk_ref, dv_ref, dq_out, dk_out, dv_out, sem):
    copies = [
        pltpu.make_async_copy(src, dst, sem.at[n])
        for n, (src, dst) in enumerate(((dq_ref, dq_out), (dk_ref, dk_out), (dv_ref, dv_out)))
    ]
    for copy in copies:
        copy.start()
    for copy in copies:
        copy.wait()


def shards(count, per_seq, query_rows, key_rows, value_rows, out_grad, logsumexp, row_delta, doc_lengths):
    rows, head = key_rows.shape
    wide = query_rows.shape
    heads = wide[1] // head
    sums = (2, rows // LANES, LANES, head)
    half, full = jnp.bfloat16, jnp.float32
    vmem = pl.BlockSpec(memory_space=pltpu.VMEM)
    hbm = pl.BlockSpec(memory_space=pl.ANY)
    operands = [
        pltpu.with_memory_space_constraint(x, pltpu.HBM)
        for x in (doc_lengths.reshape(1, -1), query_rows, out_grad, key_rows, value_rows, logsumexp, row_delta)
    ]
    grads = pl.pallas_call(
        functools.partial(kernel, count, per_seq),
        out_shape=(
            jax.ShapeDtypeStruct(wide, half),
            jax.ShapeDtypeStruct((rows, head), half),
            jax.ShapeDtypeStruct((rows, head), half),
        ),
        in_specs=[hbm] * 7,
        out_specs=(vmem, vmem, vmem),
        scratch_shapes=[
            pltpu.VMEM((1, doc_lengths.shape[0]), jnp.int32),
            pltpu.VMEM((heads * rows, head), half),
            pltpu.VMEM((heads * rows, head), half),
            pltpu.VMEM((head, heads * rows), half),
            pltpu.VMEM((head, heads * rows), half),
            pltpu.VMEM((2, rows, head), half),
            pltpu.VMEM((REACH, 2, rows, head), half),
            pltpu.VMEM((head, rows), half),
            pltpu.VMEM((rows, rows), full),
            pltpu.VMEM(logsumexp.shape, full),
            pltpu.VMEM(row_delta.shape, full),
            pltpu.VMEM((1, heads * rows), full),
            pltpu.VMEM((1, heads * rows), full),
            pltpu.VMEM((head, heads * rows), full),
            pltpu.VMEM(sums, full),
            pltpu.VMEM((REACH, *sums), full),
            pltpu.VMEM((REACH, *sums), half),
            pltpu.VMEM((2, *sums), half),
            pltpu.VMEM((2, *sums), half),
            pltpu.SemaphoreType.DMA((2, heads)),
            pltpu.SemaphoreType.DMA((5,)),
            pltpu.SemaphoreType.DMA((5,)),
            pltpu.SemaphoreType.DMA((REACH,)),
            pltpu.SemaphoreType.DMA((2,)),
            pltpu.SemaphoreType.DMA((2,)),
            pltpu.SemaphoreType.DMA((3,)),
            pltpu.SemaphoreType.DMA((3,)),
        ],
        compiler_params=pltpu.CompilerParams(
            collective_id=0, has_side_effects=True, vmem_limit_bytes=40 * MIB
        ),
    )(*operands)
    return pl.pallas_call(
        pass_on,
        out_shape=tuple(jax.ShapeDtypeStruct(x.shape, x.dtype) for x in grads),
        in_specs=[vmem] * 3,
        out_specs=(hbm,) * 3,
        scratch_shapes=[pltpu.SemaphoreType.DMA((3,))],
        compiler_params=pltpu.CompilerParams(vmem_limit_bytes=8 * MIB),
    )(*grads)


def solution(mesh):
    both = ("seq", "rep")
    count = mesh.shape["seq"] * mesh.shape["rep"]
    return jax.shard_map(
        functools.partial(shards, count, mesh.shape["rep"]),
        mesh=mesh,
        in_specs=(
            P(both, None),
            P(both, None),
            P(both, None),
            P(both, None),
            P(None, both),
            P(None, both),
            P(),
        ),
        out_specs=(P(both, None), P(both, None), P(both, None)),
        check_vma=False,
    )
```
